32 devices in a mesh: data: 1 (over z), stage: 4 (over y), tp: 8 (over x, core).
Axes of the slice: x: 4, y: 4, z: 1, core: 2. Of those that a mesh axis runs over, the one named last changes fastest.
The devices are a block of a 4x4x8 slice.
Arguments:
- x_in: bfloat16 [32, 64, 4096], P('data')
- ln_gain: bfloat16 [4, 4096], P('stage')
- w_up: bfloat16 [4, 4096, 14336], P('stage', None, 'tp')
- w_down: bfloat16 [4, 14336, 4096], P('stage', 'tp')
Outputs:
- output: bfloat16 [4, 32, 64, 4096], P('stage', 'data')
All inputs are finite; a program needn't handle non-finite values.
Results may differ from the reference program's by a relative error of at most 0.0161352.
Values are sent between devices in bfloat16 or wider.
A program may use at most 768 MiB of HBM per device.

```python
import jax
import jax.numpy as jnp
from jax import lax

D = 4096
FF = 14336
MICRO = 32
ROWS = 8
STAGES = 4
TP = 8
TOKENS = ROWS * TP
FF_SHARD = FF // TP
EPS = 1e-5


def setup_inputs(seed: int = 0, part: int = 0) -> dict:
    data_key = jax.random.fold_in(jax.random.key(seed), part)
    gain_key, up_key, down_key = jax.random.split(jax.random.key(seed + 1), 3)
    x_in = jax.random.normal(data_key, (MICRO, TOKENS, D), jnp.float32)
    ln_gain = jax.random.uniform(gain_key, (STAGES, D), jnp.float32, 0.5, 1.5)
    w_up = jax.random.normal(up_key, (STAGES, D, FF), jnp.float32) * (D ** -0.5)
    w_down = jax.random.normal(down_key, (STAGES, FF, D), jnp.float32) * (FF ** -0.5)
    return {"x_in": x_in.astype(jnp.bfloat16), "ln_gain": ln_gain.astype(jnp.bfloat16), "w_up": w_up.astype(jnp.bfloat16), "w_down": w_down.astype(jnp.bfloat16)}


def layer_norm(y_prev, ln_g):
    y_wide = y_prev.astype(jnp.float32)
    centered = y_wide - jnp.mean(y_wide, axis=-1, keepdims=True)
    variance = jnp.mean(centered * centered, axis=-1, keepdims=True)
    return (centered * lax.rsqrt(variance + EPS) * ln_g.astype(jnp.float32)).astype(jnp.bfloat16)


def stage_block(y_prev, ln_g, up_w, down_w):
    normed = layer_norm(y_prev, ln_g)
    hidden = jax.nn.gelu(jnp.dot(normed, up_w, preferred_element_type=jnp.float32), approximate=True).astype(jnp.bfloat16)
    hid_blocks = jnp.transpose(hidden.reshape(TOKENS, TP, FF_SHARD), (1, 0, 2))
    down_blocks = down_w.reshape(TP, FF_SHARD, D)

    def add_shard(running, pair):
        hid_part, down_part = pair
        partial_out = jnp.dot(hid_part, down_part, preferred_element_type=jnp.float32)
        return running + partial_out.astype(jnp.bfloat16).astype(jnp.float32), None

    total = lax.scan(add_shard, jnp.zeros((TOKENS, D), jnp.float32), (hid_blocks, down_blocks))[0]
    return (y_prev.astype(jnp.float32) + total).astype(jnp.bfloat16)


def reference(x_in, ln_gain, w_up, w_down):
    def one_micro(micro_in):
        def one_stage(y_prev, stage_weights):
            ln_g, up_w, down_w = stage_weights
            y_next = stage_block(y_prev, ln_g, up_w, down_w)
            return y_next, y_next
        return lax.scan(one_stage, micro_in, (ln_gain, w_up, w_down))[1]
    stacked = lax.map(one_micro, x_in)
    return jnp.transpose(stacked, (1, 0, 2, 3))
```

```python
import functools

import jax
import jax.numpy as jnp
from jax import lax
from jax.experimental import pallas as pl
from jax.experimental.pallas import tpu as pltpu
from jax.sharding import PartitionSpec as P

EPS = 1e-5
MESH = pl.DeviceIdType.MESH
CORES = 2
MERGE = 2
SLOTS = 3
STAGING = 3
LAG_FIRST = 13
LAG_RELAY = 6
LN_ROWS = 64
F32, BF16 = jnp.float32, jnp.bfloat16


def mlp_kernel(
    n_stage, n_tp, x_hbm, gain_ref, up_hbm, down_hbm, y_hbm,
    up, down, acts, normed, hidden, part, pair, lead, ring1, direct, ring2, carry, shard,
    w_sem, x_sem, own_r, side_r, opp_r, mate_r, back_r, relay_r, out_r,
    pair_r, ring1_r, direct_r, ring2_r,
    side_s, mate_s, fwd_s, back_s, relay_s, pair_s, ring1_s, direct_s, ring2_s, next_s, out_s, keep_s,
):
    groups, blocks, rows, width = x_hbm.shape
    half = width // 2
    chips = n_tp // CORES
    stage = lax.axis_index("stage")
    rank = lax.axis_index("tp")
    chip, core = rank // CORES, lax.rem(rank, CORES)
    first = stage == 0

    def at_chip(step):
        return lax.rem(chip + step, chips)

    right_c, left_c, opp_c = at_chip(1), at_chip(chips - 1), at_chip(2)
    mate = {"tp": chip * CORES + (1 - core)}
    right = {"tp": right_c * CORES + core}
    left = {"tp": left_c * CORES + core}
    ahead = {"stage": lax.rem(stage + 1, n_stage)}
    behind = {"stage": lax.rem(stage + n_stage - 1, n_stage)}
    block_r, block_l, block_o = right_c * CORES + core, left_c * CORES + core, opp_c * CORES + core
    cols = (pl.ds(0, half), pl.ds(half, half))

    def remote(src, dst, send, recv, device):
        return pltpu.make_async_remote_copy(
            src_ref=src, dst_ref=dst, send_sem=send, recv_sem=recv, device_id=device, device_id_type=MESH
        )

    def when_group(g):
        return pl.when((g >= 0) & (g < groups))

    barrier = pltpu.get_barrier_semaphore()
    for peer in (mate, right, left, ahead, behind):
        pl.semaphore_signal(barrier, inc=1, device_id=peer, device_id_type=MESH)

    load_up = pltpu.make_async_copy(up_hbm.at[0], up, w_sem.at[0])
    load_down = pltpu.make_async_copy(down_hbm.at[0], down, w_sem.at[1])
    load_up.start()

    def load_x(g):
        return pltpu.make_async_copy(x_hbm.at[g], acts.at[groups + lax.rem(g, STAGING)], x_sem.at[lax.rem(g, STAGING)])

    @pl.when(first)
    def _():
        load_x(0).start()

    load_down.start()
    pl.semaphore_wait(barrier, 5)

    def in_slot(g):
        return jnp.where(first, groups + lax.rem(g, STAGING), g)

    def side_copy(g, way):
        return remote(acts.at[g, rank], acts.at[g, rank], side_s.at[lax.rem(g, 4), way], side_r.at[g, way], (right, left)[way])

    def fwd_copy(g, way):
        block = (block_l, block_r)[way]
        ref = acts.at[g, block, :, cols[way]]
        return remote(ref, ref, fwd_s.at[lax.rem(g, 4), way], opp_r.at[g, way], (right, left)[way])

    def mate_copy(g, which):
        block = (rank, block_l, block_r, block_o)[which]
        return remote(acts.at[g, block], acts.at[g, block], mate_s.at[lax.rem(g, 4), which], mate_r.at[g, which], mate)

    def back_copy(g, which):
        block = (block_l, block_r, block_o)[which]
        return remote(acts.at[g, block], y_hbm.at[g, block], back_s.at[lax.rem(g, 4), which], back_r.at[g, which], behind)

    def next_copy(g):
        slot = lax.rem(g, 2)
        return remote(shard.at[slot], acts.at[g, rank], next_s.at[slot], own_r.at[g], ahead)

    def gather_own(g):
        @when_group(g)
        def _():
            next_copy(g).wait_recv()
            side_copy(g, 0).start()
            side_copy(g, 1).start()

            @pl.when(jnp.logical_not(first))
            def _():
                mate_copy(g, 0).start()

    def gather_sides(g):
        @when_group(g)
        def _():
            side_copy(g, 0).wait_recv()
            side_copy(g, 1).wait_recv()
            fwd_copy(g, 0).start()
            fwd_copy(g, 1).start()

            @pl.when(jnp.logical_not(first))
            def _():
                mate_copy(g, 1).start()
                mate_copy(g, 2).start()

            back_copy(g, 0).start()
            back_copy(g, 1).start()

    def gather_opposite(g):
        @when_group(g)
        def _():
            fwd_copy(g, 0).wait_recv()
            fwd_copy(g, 1).wait_recv()

            @pl.when(jnp.logical_not(first))
            def _():
                mate_copy(g, 3).start()

            back_copy(g, 2).start()

    def gather_mate(g):
        @pl.when((g >= 0) & (g < groups) & jnp.logical_not(first))
        def _():
            for which in range(4):
                mate_copy(g, which).wait_recv()

    def gather_sent(g):
        @when_group(g)
        def _():
            for way in range(2):
                side_copy(g, way).wait_send()
                fwd_copy(g, way).wait_send()
            for which in range(3):
                back_copy(g, which).wait_send()

            @pl.when(jnp.logical_not(first))
            def _():
                for which in range(4):
                    mate_copy(g, which).wait_send()

    def pair_copy(g, h):
        slot, to = lax.rem(g, 2), lax.rem(g, SLOTS)
        return remote(
            part.at[slot, 1 - core, :, :, cols[h]], pair.at[to, :, :, cols[h]], pair_s.at[slot, h], pair_r.at[to, h], mate
        )

    def ring1_copy(g, h):
        slot, to = lax.rem(g, 2), lax.rem(g, SLOTS)
        return remote(lead.at[slot, h, 0], ring1.at[to, h], ring1_s.at[slot, h], ring1_r.at[to, h], (right, left)[h])

    def direct_copy(g, h):
        slot, to = lax.rem(g, 2), lax.rem(g, SLOTS)
        return remote(lead.at[slot, h, 1], direct.at[to, h], direct_s.at[slot, h], direct_r.at[to, h], (left, right)[h])

    def ring2_copy(g, h):
        slot, to = lax.rem(g, 2), lax.rem(g, SLOTS)
        return remote(carry.at[slot, h], ring2.at[to, h], ring2_s.at[slot, h], ring2_r.at[to, h], (right, left)[h])

    def pair_sum(g, c, h):
        return part[lax.rem(g, 2), core, c, :, cols[h]].astype(F32) + pair[lax.rem(g, SLOTS), c, :, cols[h]].astype(F32)

    def reduce_pair(g, h):
        @when_group(g)
        def _():
            slot = lax.rem(g, 2)
            pair_copy(g, h).wait_recv()
            lead[slot, h, 0] = pair_sum(g, opp_c, h).astype(BF16)
            lead[slot, h, 1] = pair_sum(g, (left_c, right_c)[h], h).astype(BF16)
            ring1_copy(g, h).start()
            direct_copy(g, h).start()

    def reduce_ring(g):
        @when_group(g)
        def _():
            slot = lax.rem(g, 2)
            for h in range(2):
                ring1_copy(g, h).wait_recv()
                total = pair_sum(g, (right_c, left_c)[h], h) + ring1[lax.rem(g, SLOTS), h].astype(F32)
                carry[slot, h] = total.astype(BF16)
                ring2_copy(g, h).start()

    def keep_copy(g):
        slot = lax.rem(g, 2)
        return pltpu.make_async_copy(shard.at[slot], y_hbm.at[g, rank], keep_s.at[slot])

    def out_copy(g):
        slot = lax.rem(g, 2)
        return remote(shard.at[slot], y_hbm.at[g, rank], out_s.at[slot], out_r.at[g], mate)

    def reduce_last(g):
        @when_group(g)
        def _():
            slot = lax.rem(g, 2)
            for h in range(2):
                direct_copy(g, h).wait_recv()
                ring2_copy(g, h).wait_recv()
            src = in_slot(g)
            for h in range(2):
                total = pair_sum(g, chip, h) + ring2[lax.rem(g, SLOTS), h].astype(F32) + direct[lax.rem(g, SLOTS), h].astype(F32)
                shard[slot, :, cols[h]] = (acts[src, rank, :, cols[h]].astype(F32) + total).astype(BF16)
            next_copy(g).start()
            keep_copy(g).start()
            out_copy(g).start()

    def reduce_sent(g):
        @when_group(g)
        def _():
            for h in range(2):
                pair_copy(g, h).wait_send()
                ring1_copy(g, h).wait_send()
                direct_copy(g, h).wait_send()

    def shard_sent(g):
        @when_group(g)
        def _():
            for h in range(2):
                ring2_copy(g, h).wait_send()
            next_copy(g).wait_send()
            keep_copy(g).wait()
            out_copy(g).wait_send()

    def relay_copy(g, which):
        block = (block_l, block_r, block_o)[which]
        ref = y_hbm.at[g, block]
        return remote(ref, ref, relay_s.at[lax.rem(g, 4), which], relay_r.at[g, which], mate)

    def relay(g):
        @when_group(g)
        def _():
            for which in range(3):
                back_copy(g, which).wait_recv()
                relay_copy(g, which).start()

    def relay_done(g):
        @when_group(g)
        def _():
            for which in range(3):
                relay_copy(g, which).wait()
            out_copy(g).wait_recv()

    def layer_norm(g):
        src = in_slot(g)
        gain = gain_ref[...].astype(F32)
        per = LN_ROWS // rows
        for piece in range(blocks // per):
            y = acts[src, pl.ds(piece * per, per)].reshape(LN_ROWS, width).astype(F32)
            centered = y - jnp.mean(y, axis=-1, keepdims=True)
            variance = jnp.mean(centered * centered, axis=-1, keepdims=True)
            normed[pl.ds(piece * LN_ROWS, LN_ROWS), :] = (centered * lax.rsqrt(variance + EPS) * gain).astype(BF16)

    def matmul_up():
        total = jnp.dot(normed[...], up[...], preferred_element_type=F32)
        hidden[...] = jax.nn.gelu(total, approximate=True).astype(BF16)

    def matmul_down(g, h):
        slot = lax.rem(g, 2)
        total = jnp.dot(hidden[...], down[:, cols[h]], preferred_element_type=F32).astype(BF16)
        for block in range(blocks):
            part[slot, block % CORES, block // CORES, :, cols[h]] = total[block * rows:(block + 1) * rows]
        pair_copy(g, h).start()

    gather_lag = jnp.where(first, -LAG_FIRST, 2)

    def step(i):
        ag = i + gather_lag
        reduce_sent(i - 2)
        shard_sent(i - 3)
        gather_sent(ag - 4)
        relay(i - LAG_RELAY)
        relay_done(i - LAG_RELAY - 2)
        gather_mate(ag - 2)

        @when_group(i)
        def _():
            @pl.when(first)
            def _():
                load_x(i).wait()

                @pl.when(i + 1 < groups)
                def _():
                    load_x(i + 1).start()

            layer_norm(i)

        reduce_pair(i - 1, 1)

        @when_group(i)
        def _():
            @pl.when(i == 0)
            def _():
                load_up.wait()

            matmul_up()

        reduce_ring(i - 1)
        gather_sides(ag - 1)

        @when_group(i)
        def _():
            @pl.when(i == 0)
            def _():
                load_down.wait()

            matmul_down(i, 0)
            matmul_down(i, 1)

        reduce_pair(i, 0)
        reduce_last(i - 1)
        gather_opposite(ag - 1)
        gather_own(ag)

    @pl.loop(-2, groups + LAG_FIRST + 5)
    def _(i):
        step(i)


def solution(mesh):
    n_stage = mesh.shape["stage"]
    n_tp = mesh.shape["tp"]

    def per_device(x_local, gain_local, up_local, down_local):
        micro, tokens, width = x_local.shape
        inner = up_local.shape[2]
        groups, size = micro // MERGE, MERGE * tokens
        rows = size // n_tp
        chips = n_tp // CORES
        half = width // 2
        x_blocks = x_local.reshape(groups, n_tp, rows, width)
        dma = pltpu.SemaphoreType.DMA
        out = pl.pallas_call(
            functools.partial(mlp_kernel, n_stage, n_tp),
            out_shape=jax.ShapeDtypeStruct(x_blocks.shape, BF16),
            in_specs=[
                pl.BlockSpec(memory_space=pl.ANY),
                pl.BlockSpec(memory_space=pltpu.VMEM),
                pl.BlockSpec(memory_space=pl.ANY),
                pl.BlockSpec(memory_space=pl.ANY),
            ],
            out_specs=pl.BlockSpec(memory_space=pl.ANY),
            scratch_shapes=[
                pltpu.VMEM((width, inner), BF16),
                pltpu.VMEM((inner, width), BF16),
                pltpu.VMEM((groups + STAGING, n_tp, rows, width), BF16),
                pltpu.VMEM((size, width), BF16),
                pltpu.VMEM((size, inner), BF16),
                pltpu.VMEM((2, CORES, chips, rows, width), BF16),
                pltpu.VMEM((SLOTS, chips, rows, width), BF16),
                pltpu.VMEM((2, 2, 2, rows, half), BF16),
                pltpu.VMEM((SLOTS, 2, rows, half), BF16),
                pltpu.VMEM((SLOTS, 2, rows, half), BF16),
                pltpu.VMEM((SLOTS, 2, rows, half), BF16),
                pltpu.VMEM((2, 2, rows, half), BF16),
                pltpu.VMEM((2, rows, width), BF16),
                dma((2,)), dma((STAGING,)),
                dma((groups,)), dma((groups, 2)), dma((groups, 2)), dma((groups, 4)),
                dma((groups, 3)), dma((groups, 3)), dma((groups,)),
                dma((SLOTS, 2)), dma((SLOTS, 2)), dma((SLOTS, 2)), dma((SLOTS, 2)),
                dma((4, 2)), dma((4, 4)), dma((4, 2)), dma((4, 3)), dma((4, 3)),
                dma((2, 2)), dma((2, 2)), dma((2, 2)), dma((2, 2)), dma((2,)), dma((2,)), dma((2,)),
            ],
            compiler_params=pltpu.CompilerParams(
                collective_id=0, has_side_effects=True, vmem_limit_bytes=66_000_000
            ),
            name="mlp_pipeline",
        )(x_blocks, gain_local, up_local, down_local)
        return out.reshape(1, micro, tokens, width)

    return jax.shard_map(per_device, mesh=mesh, in_specs=(P("data"), P("stage"), P("stage", None, "tp"), P("stage", "tp", None)), out_specs=P("stage", "data"), check_vma=False)
```

```python
import functools

import jax
import jax.numpy as jnp
from jax import lax
from jax.experimental import pallas as pl
from jax.experimental.pallas import tpu as pltpu
from jax.sharding import PartitionSpec as P

EPS = 1e-5
MESH = pl.DeviceIdType.MESH
CORES = 2
MERGE = 2
SLOTS = 3
STAGING = 3
LAG_FIRST = 13
TAIL = 2
LAG_RELAY = 6
LN_ROWS = 64
UP_PIECES = 1
ORDER = ("mate", "norm", "up0", "ring0", "ring1", "down0", "sides", "down1", "last", "pair0", "pair1", "own", "opp")
F32, BF16 = jnp.float32, jnp.bfloat16


def mlp_kernel(
    n_stage, n_tp, x_hbm, gain_ref, up_hbm, down_hbm, y_hbm,
    up, down, acts, normed, hidden, part, pair, lead, ring1, direct, ring2, carry, shard,
    w_sem, x_sem, own_r, side_r, opp_r, mate_r, back_r, relay_r, out_r,
    pair_r, ring1_r, direct_r, ring2_r,
    side_s, mate_s, fwd_s, back_s, relay_s, pair_s, ring1_s, direct_s, ring2_s, next_s, out_s, keep_s,
    tail_r, tail_s, tail_fwd_s, tail_keep_s, tail_mate_s,
):
    groups, blocks, rows, width = x_hbm.shape
    half = width // 2
    chips = n_tp // CORES
    stage = lax.axis_index("stage")
    rank = lax.axis_index("tp")
    chip, core = rank // CORES, lax.rem(rank, CORES)
    first = stage == 0
    final = stage == n_stage - 1
    gathers = jnp.where(first, groups - TAIL, groups)

    def at_chip(step):
        return lax.rem(chip + step, chips)

    right_c, left_c, opp_c = at_chip(1), at_chip(chips - 1), at_chip(2)
    mate = {"tp": chip * CORES + (1 - core)}
    right = {"tp": right_c * CORES + core}
    left = {"tp": left_c * CORES + core}
    ahead = {"stage": lax.rem(stage + 1, n_stage)}
    behind = {"stage": lax.rem(stage + n_stage - 1, n_stage)}
    block_r, block_l, block_o = right_c * CORES + core, left_c * CORES + core, opp_c * CORES + core
    cols = (pl.ds(0, half), pl.ds(half, half))

    def remote(src, dst, send, recv, device):
        return pltpu.make_async_remote_copy(
            src_ref=src, dst_ref=dst, send_sem=send, recv_sem=recv, device_id=device, device_id_type=MESH
        )

    def when_group(g):
        return pl.when((g >= 0) & (g < groups))

    def when_gathered(g):
        return pl.when((g >= 0) & (g < gathers))

    def is_tail(g):
        return final & (g >= groups - TAIL)

    def when_tail(g):
        return pl.when(final & (g >= groups - TAIL) & (g < groups))

    barrier = pltpu.get_barrier_semaphore()
    for peer in (mate, right, left, ahead, behind):
        pl.semaphore_signal(barrier, inc=1, device_id=peer, device_id_type=MESH)

    load_up = pltpu.make_async_copy(up_hbm.at[0], up, w_sem.at[0])
    load_down = pltpu.make_async_copy(down_hbm.at[0], down, w_sem.at[1])
    load_up.start()

    def load_x(g):
        return pltpu.make_async_copy(x_hbm.at[g], acts.at[groups + lax.rem(g, STAGING)], x_sem.at[lax.rem(g, STAGING)])

    @pl.when(first)
    def _():
        load_x(0).start()

    load_down.start()
    pl.semaphore_wait(barrier, 5)

    def in_slot(g):
        return jnp.where(first, groups + lax.rem(g, STAGING), g)

    def side_copy(g, way):
        return remote(acts.at[g, rank], acts.at[g, rank], side_s.at[lax.rem(g, 4), way], side_r.at[g, way], (right, left)[way])

    def fwd_copy(g, way):
        block = (block_l, block_r)[way]
        ref = acts.at[g, block, :, cols[way]]
        return remote(ref, ref, fwd_s.at[lax.rem(g, 4), way], opp_r.at[g, way], (right, left)[way])

    def mate_copy(g, which):
        block = (rank, block_l, block_r, block_o)[which]
        return remote(acts.at[g, block], acts.at[g, block], mate_s.at[lax.rem(g, 4), which], mate_r.at[g, which], mate)

    def back_copy(g, which):
        block = (block_l, block_r, block_o)[which]
        return remote(acts.at[g, block], y_hbm.at[g, block], back_s.at[lax.rem(g, 4), which], back_r.at[g, which], behind)

    def next_copy(g):
        slot = lax.rem(g, 2)
        return remote(shard.at[slot], acts.at[g, rank], next_s.at[slot], own_r.at[g], ahead)

    def gather_own(g):
        @when_gathered(g)
        def _():
            next_copy(g).wait_recv()
            side_copy(g, 0).start()
            side_copy(g, 1).start()

            @pl.when(jnp.logical_not(first))
            def _():
                mate_copy(g, 0).start()

    def gather_sides(g):
        @when_gathered(g)
        def _():
            side_copy(g, 0).wait_recv()
            side_copy(g, 1).wait_recv()
            fwd_copy(g, 0).start()
            fwd_copy(g, 1).start()

            @pl.when(jnp.logical_not(first))
            def _():
                mate_copy(g, 1).start()
                mate_copy(g, 2).start()

            back_copy(g, 0).start()
            back_copy(g, 1).start()

    def gather_opposite(g):
        @when_gathered(g)
        def _():
            fwd_copy(g, 0).wait_recv()
            fwd_copy(g, 1).wait_recv()

            @pl.when(jnp.logical_not(first))
            def _():
                mate_copy(g, 3).start()

            back_copy(g, 2).start()

    def gather_mate(g):
        @pl.when((g >= 0) & (g < groups) & jnp.logical_not(first))
        def _():
            for which in range(4):
                mate_copy(g, which).wait_recv()

    def gather_sent(g):
        @when_gathered(g)
        def _():
            for way in range(2):
                side_copy(g, way).wait_send()
                fwd_copy(g, way).wait_send()
            for which in range(3):
                back_copy(g, which).wait_send()

            @pl.when(jnp.logical_not(first))
            def _():
                for which in range(4):
                    mate_copy(g, which).wait_send()

    def pair_copy(g, h):
        slot, to = lax.rem(g, 2), lax.rem(g, SLOTS)
        return remote(
            part.at[slot, 1 - core, :, :, cols[h]], pair.at[to, :, :, cols[h]], pair_s.at[slot, h], pair_r.at[to, h], mate
        )

    def ring1_copy(g, h):
        slot, to = lax.rem(g, 2), lax.rem(g, SLOTS)
        return remote(lead.at[slot, h, 0], ring1.at[to, h], ring1_s.at[slot, h], ring1_r.at[to, h], (right, left)[h])

    def direct_copy(g, h):
        slot, to = lax.rem(g, 2), lax.rem(g, SLOTS)
        return remote(lead.at[slot, h, 1], direct.at[to, h], direct_s.at[slot, h], direct_r.at[to, h], (left, right)[h])

    def ring2_copy(g, h):
        slot, to = lax.rem(g, 2), lax.rem(g, SLOTS)
        return remote(carry.at[slot, h], ring2.at[to, h], ring2_s.at[slot, h], ring2_r.at[to, h], (right, left)[h])

    def pair_sum(g, c, h):
        return part[lax.rem(g, 2), core, c, :, cols[h]].astype(F32) + pair[lax.rem(g, SLOTS), c, :, cols[h]].astype(F32)

    def reduce_pair(g, h):
        @when_group(g)
        def _():
            slot = lax.rem(g, 2)
            pair_copy(g, h).wait_recv()
            lead[slot, h, 0] = pair_sum(g, opp_c, h).astype(BF16)
            lead[slot, h, 1] = pair_sum(g, (left_c, right_c)[h], h).astype(BF16)
            ring1_copy(g, h).start()
            direct_copy(g, h).start()

    def reduce_ring(g, h):
        @when_group(g)
        def _():
            slot = lax.rem(g, 2)
            ring1_copy(g, h).wait_recv()
            total = pair_sum(g, (right_c, left_c)[h], h) + ring1[lax.rem(g, SLOTS), h].astype(F32)
            carry[slot, h] = total.astype(BF16)
            ring2_copy(g, h).start()

    def tail_side_copy(g, way):
        index = g - (groups - TAIL)
        return remote(
            shard.at[lax.rem(g, 2)], acts.at[g + TAIL, rank], tail_s.at[index, way], tail_r.at[index, way], (right, left)[way]
        )

    def tail_fwd_copy(g, way):
        index = g - (groups - TAIL)
        ref = acts.at[g + TAIL, (block_l, block_r)[way], :, cols[way]]
        return remote(ref, ref, tail_fwd_s.at[index, way], tail_r.at[index, 2 + way], (right, left)[way])

    def tail_keep_copy(g, which):
        index, block = g - (groups - TAIL), (block_l, block_r, block_o)[which]
        return pltpu.make_async_copy(acts.at[g + TAIL, block], y_hbm.at[g, block], tail_keep_s.at[index, which])

    def tail_mate_copy(g, which):
        index, block = g - (groups - TAIL), (block_l, block_r, block_o)[which]
        return remote(acts.at[g + TAIL, block], y_hbm.at[g, block], tail_mate_s.at[index, which], relay_r.at[g, which], mate)

    def tail_own(g):
        @when_tail(g)
        def _():
            tail_side_copy(g, 0).start()
            tail_side_copy(g, 1).start()

    def tail_sides(g):
        @when_tail(g)
        def _():
            for way in range(2):
                tail_side_copy(g, way).wait_recv()
                tail_fwd_copy(g, way).start()
            for which in range(2):
                tail_mate_copy(g, which).start()
                tail_keep_copy(g, which).start()

    def tail_opposite(g):
        @when_tail(g)
        def _():
            for way in range(2):
                tail_fwd_copy(g, way).wait_recv()
            tail_mate_copy(g, 2).start()
            tail_keep_copy(g, 2).start()

    def tail_done(g):
        @when_tail(g)
        def _():
            for way in range(2):
                tail_fwd_copy(g, way).wait_send()
            for which in range(3):
                tail_mate_copy(g, which).wait_send()
                tail_keep_copy(g, which).wait()

    def keep_copy(g):
        slot = lax.rem(g, 2)
        return pltpu.make_async_copy(shard.at[slot], y_hbm.at[g, rank], keep_s.at[slot])

    def out_copy(g):
        slot = lax.rem(g, 2)
        return remote(shard.at[slot], y_hbm.at[g, rank], out_s.at[slot], out_r.at[g], mate)

    def reduce_last(g):
        @when_group(g)
        def _():
            slot = lax.rem(g, 2)
            for h in range(2):
                direct_copy(g, h).wait_recv()
                ring2_copy(g, h).wait_recv()
            src = in_slot(g)
            for h in range(2):
                total = pair_sum(g, chip, h) + ring2[lax.rem(g, SLOTS), h].astype(F32) + direct[lax.rem(g, SLOTS), h].astype(F32)
                shard[slot, :, cols[h]] = (acts[src, rank, :, cols[h]].astype(F32) + total).astype(BF16)
            @pl.when(jnp.logical_not(is_tail(g)))
            def _():
                next_copy(g).start()

            keep_copy(g).start()
            out_copy(g).start()

    def reduce_sent(g):
        @when_group(g)
        def _():
            for h in range(2):
                pair_copy(g, h).wait_send()
                ring1_copy(g, h).wait_send()
                direct_copy(g, h).wait_send()

    def shard_sent(g):
        @when_group(g)
        def _():
            for h in range(2):
                ring2_copy(g, h).wait_send()

            @pl.when(jnp.logical_not(is_tail(g)))
            def _():
                next_copy(g).wait_send()

            @pl.when(is_tail(g))
            def _():
                tail_side_copy(g, 0).wait_send()
                tail_side_copy(g, 1).wait_send()

            keep_copy(g).wait()
            out_copy(g).wait_send()

    def relay_copy(g, which):
        block = (block_l, block_r, block_o)[which]
        ref = y_hbm.at[g, block]
        return remote(ref, ref, relay_s.at[lax.rem(g, 4), which], relay_r.at[g, which], mate)

    def relay(g):
        @pl.when((g >= 0) & (g < groups) & jnp.logical_not(is_tail(g)))
        def _():
            for which in range(3):
                back_copy(g, which).wait_recv()
                relay_copy(g, which).start()

    def relay_done(g):
        @when_group(g)
        def _():
            for which in range(3):
                relay_copy(g, which).wait_recv()

                @pl.when(jnp.logical_not(is_tail(g)))
                def _():
                    relay_copy(g, which).wait_send()

            out_copy(g).wait_recv()

    def layer_norm(g):
        src = in_slot(g)
        gain = gain_ref[...].astype(F32)
        per = LN_ROWS // rows
        for piece in range(blocks // per):
            y = acts[src, pl.ds(piece * per, per)].reshape(LN_ROWS, width).astype(F32)
            centered = y - jnp.mean(y, axis=-1, keepdims=True)
            variance = jnp.mean(centered * centered, axis=-1, keepdims=True)
            normed[pl.ds(piece * LN_ROWS, LN_ROWS), :] = (centered * lax.rsqrt(variance + EPS) * gain).astype(BF16)

    def matmul_up(piece):
        part_cols = pl.ds(piece * (hidden.shape[1] // UP_PIECES), hidden.shape[1] // UP_PIECES)
        total = jnp.dot(normed[...], up[:, part_cols], preferred_element_type=F32)
        hidden[:, part_cols] = jax.nn.gelu(total, approximate=True).astype(BF16)

    def matmul_down(g, h):
        slot = lax.rem(g, 2)
        total = jnp.dot(hidden[...], down[:, cols[h]], preferred_element_type=F32).astype(BF16)
        for block in range(blocks):
            part[slot, block % CORES, block // CORES, :, cols[h]] = total[block * rows:(block + 1) * rows]
        pair_copy(g, h).start()

    gather_lag = jnp.where(first, -LAG_FIRST, 2)

    def compute_norm(i):
        @when_group(i)
        def _():
            @pl.when(first)
            def _():
                load_x(i).wait()

                @pl.when(i + 1 < groups)
                def _():
                    load_x(i + 1).start()

            layer_norm(i)

    def compute_up(i, piece):
        @when_group(i)
        def _():
            @pl.when(i == 0)
            def _():
                if piece == 0:
                    load_up.wait()

            matmul_up(piece)

    def compute_down(i, h):
        @when_group(i)
        def _():
            @pl.when(i == 0)
            def _():
                if h == 0:
                    load_down.wait()

            matmul_down(i, h)

    def step(i):
        ag = i + gather_lag
        reduce_sent(i - 2)
        shard_sent(i - 3)
        gather_sent(ag - 4)
        relay(i - LAG_RELAY)
        relay_done(i - LAG_RELAY - 2)
        tail_done(i - 4)
        actions = {
            "mate": lambda: gather_mate(ag - 2),
            "norm": lambda: compute_norm(i),
            "up0": lambda: compute_up(i, 0),
            "up1": lambda: compute_up(i, 1),
            "down0": lambda: compute_down(i, 0),
            "down1": lambda: compute_down(i, 1),
            "pair0": lambda: reduce_pair(i, 0),
            "pair1": lambda: reduce_pair(i, 1),
            "pair1x": lambda: reduce_pair(i - 1, 1),
            "ring0": lambda: reduce_ring(i - 1, 0),
            "ring1": lambda: reduce_ring(i - 1, 1),
            "last": lambda: reduce_last(i - 1),
            "own": lambda: (gather_own(ag), tail_own(i - 1)),
            "sides": lambda: (gather_sides(ag - 1), tail_sides(i - 2)),
            "opp": lambda: (gather_opposite(ag - 1), tail_opposite(i - 2)),
        }
        for name in ORDER:
            actions[name]()

    @pl.loop(-2, groups + jnp.where(first, LAG_FIRST + 5 - TAIL, LAG_RELAY + 3))
    def _(i):
        step(i)


def keep_kernel(src, dst, held, in_sem, out_sem):
    groups = src.shape[0]
    reads = [pltpu.make_async_copy(src.at[g], held.at[g], in_sem.at[g]) for g in range(groups)]
    writes = [pltpu.make_async_copy(held.at[g], dst.at[g], out_sem.at[g]) for g in range(groups)]
    for copy in reads:
        copy.start()
    for g in range(groups):
        reads[g].wait()
        writes[g].start()
    for copy in writes:
        copy.wait()


def solution(mesh):
    n_stage = mesh.shape["stage"]
    n_tp = mesh.shape["tp"]

    def per_device(x_local, gain_local, up_local, down_local):
        micro, tokens, width = x_local.shape
        inner = up_local.shape[2]
        groups, size = micro // MERGE, MERGE * tokens
        rows = size // n_tp
        chips = n_tp // CORES
        half = width // 2
        x_blocks = x_local.reshape(groups, n_tp, rows, width)
        dma = pltpu.SemaphoreType.DMA
        out = pl.pallas_call(
            functools.partial(mlp_kernel, n_stage, n_tp),
            out_shape=jax.ShapeDtypeStruct(x_blocks.shape, BF16),
            in_specs=[
                pl.BlockSpec(memory_space=pl.ANY),
                pl.BlockSpec(memory_space=pltpu.VMEM),
                pl.BlockSpec(memory_space=pl.ANY),
                pl.BlockSpec(memory_space=pl.ANY),
            ],
            out_specs=pl.BlockSpec(memory_space=pl.ANY),
            scratch_shapes=[
                pltpu.VMEM((width, inner), BF16),
                pltpu.VMEM((inner, width), BF16),
                pltpu.VMEM((groups + STAGING, n_tp, rows, width), BF16),
                pltpu.VMEM((size, width), BF16),
                pltpu.VMEM((size, inner), BF16),
                pltpu.VMEM((2, CORES, chips, rows, width), BF16),
                pltpu.VMEM((SLOTS, chips, rows, width), BF16),
                pltpu.VMEM((2, 2, 2, rows, half), BF16),
                pltpu.VMEM((SLOTS, 2, rows, half), BF16),
                pltpu.VMEM((SLOTS, 2, rows, half), BF16),
                pltpu.VMEM((SLOTS, 2, rows, half), BF16),
                pltpu.VMEM((2, 2, rows, half), BF16),
                pltpu.VMEM((2, rows, width), BF16),
                dma((2,)), dma((STAGING,)),
                dma((groups,)), dma((groups, 2)), dma((groups, 2)), dma((groups, 4)),
                dma((groups, 3)), dma((groups, 3)), dma((groups,)),
                dma((SLOTS, 2)), dma((SLOTS, 2)), dma((SLOTS, 2)), dma((SLOTS, 2)),
                dma((4, 2)), dma((4, 4)), dma((4, 2)), dma((4, 3)), dma((4, 3)),
                dma((2, 2)), dma((2, 2)), dma((2, 2)), dma((2, 2)), dma((2,)), dma((2,)), dma((2,)),
                dma((TAIL, 4)), dma((TAIL, 2)), dma((TAIL, 2)), dma((TAIL, 3)), dma((TAIL, 3)),
            ],
            compiler_params=pltpu.CompilerParams(
                collective_id=0, has_side_effects=True, vmem_limit_bytes=66_000_000
            ),
            name="mlp_pipeline",
        )(x_blocks, gain_local, up_local, down_local)
        kept = pl.pallas_call(
            keep_kernel,
            out_shape=jax.ShapeDtypeStruct(x_blocks.shape, BF16),
            in_specs=[pl.BlockSpec(memory_space=pl.ANY)],
            out_specs=pl.BlockSpec(memory_space=pl.ANY),
            scratch_shapes=[pltpu.VMEM(x_blocks.shape, BF16), dma((groups,)), dma((groups,))],
            compiler_params=pltpu.CompilerParams(vmem_limit_bytes=40_000_000),
            name="keep_result",
        )(out)
        return kept.reshape(1, micro, tokens, width)

    return jax.shard_map(per_device, mesh=mesh, in_specs=(P("data"), P("stage"), P("stage", None, "tp"), P("stage", "tp", None)), out_specs=P("stage", "data"), check_vma=False)
```

```python
import functools

import jax
import jax.numpy as jnp
from jax import lax
from jax.experimental import pallas as pl
from jax.experimental.pallas import tpu as pltpu
from jax.sharding import PartitionSpec as P

EPS = 1e-5
MESH = pl.DeviceIdType.MESH
CORES = 2
MERGE = 2
SLOTS = 3
STAGING = 3
LAG_FIRST = 13
TAIL = 2
LAG_RELAY = 6
LN_ROWS = 64
UP_PIECES = 1
ORDER = ("mate", "own", "norm", "up0", "ring0", "ring1", "down0", "sides", "rest", "down1", "pair0", "last", "pair1", "opp")
F32, BF16 = jnp.float32, jnp.bfloat16


def mlp_kernel(
    n_stage, n_tp, x_hbm, gain_ref, up_hbm, down_hbm, y_hbm,
    up, down, acts, normed, hidden, part, pair, lead, ring1, direct, ring2, carry, shard,
    w_sem, x_sem, own_r, side_r, opp_r, mate_r, back_r, relay_r, out_r,
    pair_r, ring1_r, direct_r, ring2_r,
    side_s, mate_s, fwd_s, back_s, relay_s, pair_s, ring1_s, direct_s, ring2_s, next_s, out_s, keep_s,
    tail_r, tail_s, tail_fwd_s, tail_keep_s, tail_mate_s,
):
    groups, blocks, rows, width = x_hbm.shape
    half = width // 2
    chips = n_tp // CORES
    stage = lax.axis_index("stage")
    rank = lax.axis_index("tp")
    chip, core = rank // CORES, lax.rem(rank, CORES)
    first = stage == 0
    final = stage == n_stage - 1
    gathers = jnp.where(first, groups - TAIL, groups)

    def at_chip(step):
        return lax.rem(chip + step, chips)

    right_c, left_c, opp_c = at_chip(1), at_chip(chips - 1), at_chip(2)
    mate = {"tp": chip * CORES + (1 - core)}
    right = {"tp": right_c * CORES + core}
    left = {"tp": left_c * CORES + core}
    ahead = {"stage": lax.rem(stage + 1, n_stage)}
    behind = {"stage": lax.rem(stage + n_stage - 1, n_stage)}
    block_r, block_l, block_o = right_c * CORES + core, left_c * CORES + core, opp_c * CORES + core
    cols = (pl.ds(0, half), pl.ds(half, half))

    def remote(src, dst, send, recv, device):
        return pltpu.make_async_remote_copy(
            src_ref=src, dst_ref=dst, send_sem=send, recv_sem=recv, device_id=device, device_id_type=MESH
        )

    def when_group(g):
        return pl.when((g >= 0) & (g < groups))

    def when_gathered(g):
        return pl.when((g >= 0) & (g < gathers))

    def is_tail(g):
        return final & (g >= groups - TAIL)

    def when_tail(g):
        return pl.when(final & (g >= groups - TAIL) & (g < groups))

    barrier = pltpu.get_barrier_semaphore()
    for peer in (mate, right, left, ahead, behind):
        pl.semaphore_signal(barrier, inc=1, device_id=peer, device_id_type=MESH)

    load_up = pltpu.make_async_copy(up_hbm.at[0], up, w_sem.at[0])
    load_down = pltpu.make_async_copy(down_hbm.at[0], down, w_sem.at[1])
    load_up.start()

    def load_x(g):
        return pltpu.make_async_copy(x_hbm.at[g], acts.at[groups + lax.rem(g, STAGING)], x_sem.at[lax.rem(g, STAGING)])

    @pl.when(first)
    def _():
        load_x(0).start()

    load_down.start()
    pl.semaphore_wait(barrier, 5)

    def in_slot(g):
        return jnp.where(first, groups + lax.rem(g, STAGING), g)

    def side_copy(g, way, h):
        ref = acts.at[g, rank, :, cols[h]]
        return remote(ref, ref, side_s.at[lax.rem(g, 4), way, h], side_r.at[g, way, h], (right, left)[way])

    def fwd_copy(g, way):
        block = (block_l, block_r)[way]
        ref = acts.at[g, block, :, cols[way]]
        return remote(ref, ref, fwd_s.at[lax.rem(g, 4), way], opp_r.at[g, way], (right, left)[way])

    def mate_copy(g, which):
        block = (rank, block_l, block_r, block_o)[which]
        return remote(acts.at[g, block], acts.at[g, block], mate_s.at[lax.rem(g, 4), which], mate_r.at[g, which], mate)

    def back_copy(g, which):
        block = (block_l, block_r, block_o)[which]
        return remote(acts.at[g, block], y_hbm.at[g, block], back_s.at[lax.rem(g, 4), which], back_r.at[g, which], behind)

    def next_copy(g):
        slot = lax.rem(g, 2)
        return remote(shard.at[slot], acts.at[g, rank], next_s.at[slot], own_r.at[g], ahead)

    def gather_own(g):
        @when_gathered(g)
        def _():
            next_copy(g).wait_recv()
            side_copy(g, 0, 0).start()
            side_copy(g, 1, 1).start()
            side_copy(g, 0, 1).start()
            side_copy(g, 1, 0).start()

            @pl.when(jnp.logical_not(first))
            def _():
                mate_copy(g, 0).start()

    def gather_sides(g):
        @when_gathered(g)
        def _():
            for way in range(2):
                side_copy(g, way, way).wait_recv()
                fwd_copy(g, way).start()

    def gather_rest(g):
        @when_gathered(g)
        def _():
            for way in range(2):
                side_copy(g, way, 1 - way).wait_recv()

            @pl.when(jnp.logical_not(first))
            def _():
                mate_copy(g, 1).start()
                mate_copy(g, 2).start()

            back_copy(g, 0).start()
            back_copy(g, 1).start()

    def gather_opposite(g):
        @when_gathered(g)
        def _():
            fwd_copy(g, 0).wait_recv()
            fwd_copy(g, 1).wait_recv()

            @pl.when(jnp.logical_not(first))
            def _():
                mate_copy(g, 3).start()

            back_copy(g, 2).start()

    def gather_mate(g):
        @pl.when((g >= 0) & (g < groups) & jnp.logical_not(first))
        def _():
            for which in range(4):
                mate_copy(g, which).wait_recv()

    def gather_sent(g):
        @when_gathered(g)
        def _():
            for way in range(2):
                side_copy(g, way, 0).wait_send()
                side_copy(g, way, 1).wait_send()
                fwd_copy(g, way).wait_send()
            for which in range(3):
                back_copy(g, which).wait_send()

            @pl.when(jnp.logical_not(first))
            def _():
                for which in range(4):
                    mate_copy(g, which).wait_send()

    def pair_copy(g, h):
        slot, to = lax.rem(g, 2), lax.rem(g, SLOTS)
        return remote(
            part.at[slot, 1 - core, :, :, cols[h]], pair.at[to, :, :, cols[h]], pair_s.at[slot, h], pair_r.at[to, h], mate
        )

    def ring1_copy(g, h):
        slot, to = lax.rem(g, 2), lax.rem(g, SLOTS)
        return remote(lead.at[slot, h, 0], ring1.at[to, h], ring1_s.at[slot, h], ring1_r.at[to, h], (right, left)[h])

    def direct_copy(g, h):
        slot, to = lax.rem(g, 2), lax.rem(g, SLOTS)
        return remote(lead.at[slot, h, 1], direct.at[to, h], direct_s.at[slot, h], direct_r.at[to, h], (left, right)[h])

    def ring2_copy(g, h):
        slot, to = lax.rem(g, 2), lax.rem(g, SLOTS)
        return remote(carry.at[slot, h], ring2.at[to, h], ring2_s.at[slot, h], ring2_r.at[to, h], (right, left)[h])

    def pair_sum(g, c, h):
        return part[lax.rem(g, 2), core, c, :, cols[h]].astype(F32) + pair[lax.rem(g, SLOTS), c, :, cols[h]].astype(F32)

    def reduce_pair(g, h):
        @when_group(g)
        def _():
            slot = lax.rem(g, 2)
            pair_copy(g, h).wait_recv()
            lead[slot, h, 0] = pair_sum(g, opp_c, h).astype(BF16)
            lead[slot, h, 1] = pair_sum(g, (left_c, right_c)[h], h).astype(BF16)
            ring1_copy(g, h).start()
            direct_copy(g, h).start()

    def reduce_ring(g, h):
        @when_group(g)
        def _():
            slot = lax.rem(g, 2)
            ring1_copy(g, h).wait_recv()
            total = pair_sum(g, (right_c, left_c)[h], h) + ring1[lax.rem(g, SLOTS), h].astype(F32)
            carry[slot, h] = total.astype(BF16)
            ring2_copy(g, h).start()

    def tail_side_copy(g, way):
        index = g - (groups - TAIL)
        return remote(
            shard.at[lax.rem(g, 2)], acts.at[g + TAIL, rank], tail_s.at[index, way], tail_r.at[index, way], (right, left)[way]
        )

    def tail_fwd_copy(g, way):
        index = g - (groups - TAIL)
        ref = acts.at[g + TAIL, (block_l, block_r)[way], :, cols[way]]
        return remote(ref, ref, tail_fwd_s.at[index, way], tail_r.at[index, 2 + way], (right, left)[way])

    def tail_keep_copy(g, which):
        index, block = g - (groups - TAIL), (block_l, block_r, block_o)[which]
        return pltpu.make_async_copy(acts.at[g + TAIL, block], y_hbm.at[g, block], tail_keep_s.at[index, which])

    def tail_mate_copy(g, which):
        index, block = g - (groups - TAIL), (block_l, block_r, block_o)[which]
        return remote(acts.at[g + TAIL, block], y_hbm.at[g, block], tail_mate_s.at[index, which], relay_r.at[g, which], mate)

    def tail_own(g):
        @when_tail(g)
        def _():
            tail_side_copy(g, 0).start()
            tail_side_copy(g, 1).start()

    def tail_sides(g):
        @when_tail(g)
        def _():
            for way in range(2):
                tail_side_copy(g, way).wait_recv()
                tail_fwd_copy(g, way).start()
            for which in range(2):
                tail_mate_copy(g, which).start()
                tail_keep_copy(g, which).start()

    def tail_opposite(g):
        @when_tail(g)
        def _():
            for way in range(2):
                tail_fwd_copy(g, way).wait_recv()
            tail_mate_copy(g, 2).start()
            tail_keep_copy(g, 2).start()

    def tail_done(g):
        @when_tail(g)
        def _():
            for way in range(2):
                tail_fwd_copy(g, way).wait_send()
            for which in range(3):
                tail_mate_copy(g, which).wait_send()
                tail_keep_copy(g, which).wait()

    def keep_copy(g):
        slot = lax.rem(g, 2)
        return pltpu.make_async_copy(shard.at[slot], y_hbm.at[g, rank], keep_s.at[slot])

    def out_copy(g):
        slot = lax.rem(g, 2)
        return remote(shard.at[slot], y_hbm.at[g, rank], out_s.at[slot], out_r.at[g], mate)

    def reduce_last(g):
        @when_group(g)
        def _():
            slot = lax.rem(g, 2)
            for h in range(2):
                direct_copy(g, h).wait_recv()
                ring2_copy(g, h).wait_recv()
            src = in_slot(g)
            for h in range(2):
                total = pair_sum(g, chip, h) + ring2[lax.rem(g, SLOTS), h].astype(F32) + direct[lax.rem(g, SLOTS), h].astype(F32)
                shard[slot, :, cols[h]] = (acts[src, rank, :, cols[h]].astype(F32) + total).astype(BF16)
            @pl.when(jnp.logical_not(is_tail(g)))
            def _():
                next_copy(g).start()

            keep_copy(g).start()
            out_copy(g).start()

    def reduce_sent(g):
        @when_group(g)
        def _():
            for h in range(2):
                pair_copy(g, h).wait_send()
                ring1_copy(g, h).wait_send()
                direct_copy(g, h).wait_send()

    def shard_sent(g):
        @when_group(g)
        def _():
            for h in range(2):
                ring2_copy(g, h).wait_send()

            @pl.when(jnp.logical_not(is_tail(g)))
            def _():
                next_copy(g).wait_send()

            @pl.when(is_tail(g))
            def _():
                tail_side_copy(g, 0).wait_send()
                tail_side_copy(g, 1).wait_send()

            keep_copy(g).wait()
            out_copy(g).wait_send()

    def relay_copy(g, which):
        block = (block_l, block_r, block_o)[which]
        ref = y_hbm.at[g, block]
        return remote(ref, ref, relay_s.at[lax.rem(g, 4), which], relay_r.at[g, which], mate)

    def relay(g):
        @pl.when((g >= 0) & (g < groups) & jnp.logical_not(is_tail(g)))
        def _():
            for which in range(3):
                back_copy(g, which).wait_recv()
                relay_copy(g, which).start()

    def relay_done(g):
        @when_group(g)
        def _():
            for which in range(3):
                relay_copy(g, which).wait_recv()

                @pl.when(jnp.logical_not(is_tail(g)))
                def _():
                    relay_copy(g, which).wait_send()

            out_copy(g).wait_recv()

    def layer_norm(g):
        src = in_slot(g)
        gain = gain_ref[...].astype(F32)
        per = LN_ROWS // rows
        for piece in range(blocks // per):
            y = acts[src, pl.ds(piece * per, per)].reshape(LN_ROWS, width).astype(F32)
            centered = y - jnp.mean(y, axis=-1, keepdims=True)
            variance = jnp.mean(centered * centered, axis=-1, keepdims=True)
            normed[pl.ds(piece * LN_ROWS, LN_ROWS), :] = (centered * lax.rsqrt(variance + EPS) * gain).astype(BF16)

    def matmul_up(piece):
        part_cols = pl.ds(piece * (hidden.shape[1] // UP_PIECES), hidden.shape[1] // UP_PIECES)
        total = jnp.dot(normed[...], up[:, part_cols], preferred_element_type=F32)
        hidden[:, part_cols] = jax.nn.gelu(total, approximate=True).astype(BF16)

    def matmul_down(g, h):
        slot = lax.rem(g, 2)
        total = jnp.dot(hidden[...], down[:, cols[h]], preferred_element_type=F32).astype(BF16)
        for block in range(blocks):
            part[slot, block % CORES, block // CORES, :, cols[h]] = total[block * rows:(block + 1) * rows]
        pair_copy(g, h).start()

    gather_lag = jnp.where(first, -LAG_FIRST, 2)

    def compute_norm(i):
        @when_group(i)
        def _():
            @pl.when(first)
            def _():
                load_x(i).wait()

                @pl.when(i + 1 < groups)
                def _():
                    load_x(i + 1).start()

            layer_norm(i)

    def compute_up(i, piece):
        @when_group(i)
        def _():
            @pl.when(i == 0)
            def _():
                if piece == 0:
                    load_up.wait()

            matmul_up(piece)

    def compute_down(i, h):
        @when_group(i)
        def _():
            @pl.when(i == 0)
            def _():
                if h == 0:
                    load_down.wait()

            matmul_down(i, h)

    def step(i):
        ag = i + gather_lag
        reduce_sent(i - 2)
        shard_sent(i - 3)
        gather_sent(ag - 4)
        relay(i - LAG_RELAY)
        relay_done(i - LAG_RELAY - 2)
        tail_done(i - 4)
        actions = {
            "mate": lambda: gather_mate(ag - 2),
            "norm": lambda: compute_norm(i),
            "up0": lambda: compute_up(i, 0),
            "down0": lambda: compute_down(i, 0),
            "down1": lambda: compute_down(i, 1),
            "pair0": lambda: reduce_pair(i, 0),
            "pair1": lambda: reduce_pair(i, 1),
            "ring0": lambda: reduce_ring(i - 1, 0),
            "ring1": lambda: reduce_ring(i - 1, 1),
            "last": lambda: reduce_last(i - 1),
            "own": lambda: (gather_own(ag - 1), tail_own(i - 2)),
            "sides": lambda: (gather_sides(ag - 1), tail_sides(i - 2)),
            "rest": lambda: gather_rest(ag - 1),
            "opp": lambda: (gather_opposite(ag - 1), tail_opposite(i - 2)),
        }
        for name in ORDER:
            actions[name]()

    @pl.loop(-2, groups + jnp.where(first, LAG_FIRST + 5 - TAIL, LAG_RELAY + 3))
    def _(i):
        step(i)


def keep_kernel(src, dst, held, in_sem, out_sem):
    groups = src.shape[0]
    reads = [pltpu.make_async_copy(src.at[g], held.at[g], in_sem.at[g]) for g in range(groups)]
    writes = [pltpu.make_async_copy(held.at[g], dst.at[g], out_sem.at[g]) for g in range(groups)]
    for copy in reads:
        copy.start()
    for g in range(groups):
        reads[g].wait()
        writes[g].start()
    for copy in writes:
        copy.wait()


def solution(mesh):
    n_stage = mesh.shape["stage"]
    n_tp = mesh.shape["tp"]

    def per_device(x_local, gain_local, up_local, down_local):
        micro, tokens, width = x_local.shape
        inner = up_local.shape[2]
        groups, size = micro // MERGE, MERGE * tokens
        rows = size // n_tp
        chips = n_tp // CORES
        half = width // 2
        x_blocks = x_local.reshape(groups, n_tp, rows, width)
        dma = pltpu.SemaphoreType.DMA
        out = pl.pallas_call(
            functools.partial(mlp_kernel, n_stage, n_tp),
            out_shape=jax.ShapeDtypeStruct(x_blocks.shape, BF16),
            in_specs=[
                pl.BlockSpec(memory_space=pl.ANY),
                pl.BlockSpec(memory_space=pltpu.VMEM),
                pl.BlockSpec(memory_space=pl.ANY),
                pl.BlockSpec(memory_space=pl.ANY),
            ],
            out_specs=pl.BlockSpec(memory_space=pl.ANY),
            scratch_shapes=[
                pltpu.VMEM((width, inner), BF16),
                pltpu.VMEM((inner, width), BF16),
                pltpu.VMEM((groups + STAGING, n_tp, rows, width), BF16),
                pltpu.VMEM((size, width), BF16),
                pltpu.VMEM((size, inner), BF16),
                pltpu.VMEM((2, CORES, chips, rows, width), BF16),
                pltpu.VMEM((SLOTS, chips, rows, width), BF16),
                pltpu.VMEM((2, 2, 2, rows, half), BF16),
                pltpu.VMEM((SLOTS, 2, rows, half), BF16),
                pltpu.VMEM((SLOTS, 2, rows, half), BF16),
                pltpu.VMEM((SLOTS, 2, rows, half), BF16),
                pltpu.VMEM((2, 2, rows, half), BF16),
                pltpu.VMEM((2, rows, width), BF16),
                dma((2,)), dma((STAGING,)),
                dma((groups,)), dma((groups, 2, 2)), dma((groups, 2)), dma((groups, 4)),
                dma((groups, 3)), dma((groups, 3)), dma((groups,)),
                dma((SLOTS, 2)), dma((SLOTS, 2)), dma((SLOTS, 2)), dma((SLOTS, 2)),
                dma((4, 2, 2)), dma((4, 4)), dma((4, 2)), dma((4, 3)), dma((4, 3)),
                dma((2, 2)), dma((2, 2)), dma((2, 2)), dma((2, 2)), dma((2,)), dma((2,)), dma((2,)),
                dma((TAIL, 4)), dma((TAIL, 2)), dma((TAIL, 2)), dma((TAIL, 3)), dma((TAIL, 3)),
            ],
            compiler_params=pltpu.CompilerParams(
                collective_id=0, has_side_effects=True, vmem_limit_bytes=66_000_000
            ),
            name="mlp_pipeline",
        )(x_blocks, gain_local, up_local, down_local)
        kept = pl.pallas_call(
            keep_kernel,
            out_shape=jax.ShapeDtypeStruct(x_blocks.shape, BF16),
            in_specs=[pl.BlockSpec(memory_space=pl.ANY)],
            out_specs=pl.BlockSpec(memory_space=pl.ANY),
            scratch_shapes=[pltpu.VMEM(x_blocks.shape, BF16), dma((groups,)), dma((groups,))],
            compiler_params=pltpu.CompilerParams(vmem_limit_bytes=40_000_000),
            name="keep_result",
        )(out)
        return kept.reshape(1, micro, tokens, width)

    return jax.shard_map(per_device, mesh=mesh, in_specs=(P("data"), P("stage"), P("stage", None, "tp"), P("stage", "tp", None)), out_specs=P("stage", "data"), check_vma=False)
```

```python
import functools

import jax
import jax.numpy as jnp
from jax import lax
from jax.experimental import pallas as pl
from jax.experimental.pallas import tpu as pltpu
from jax.sharding import PartitionSpec as P

EPS = 1e-5
MESH = pl.DeviceIdType.MESH
CORES = 2
MERGE = 2
SLOTS = 3
STAGING = 3
LAG_FIRST = 13
TAIL = 2
LAG_RELAY = 5
LN_ROWS = 64
UP_PIECES = 1
ORDER = ("mate", "own", "norm", "up0", "ring0", "ring1", "down0", "sides", "down1", "pair0", "rest", "last", "pair1", "opp")
F32, BF16 = jnp.float32, jnp.bfloat16


def mlp_kernel(
    n_stage, n_tp, x_hbm, gain_ref, up_hbm, down_hbm, y_hbm,
    up, down, acts, normed, hidden, part, pair, lead, ring1, direct, ring2, carry, shard,
    w_sem, x_sem, own_r, side_r, opp_r, mate_r, back_r, relay_r, out_r,
    pair_r, ring1_r, direct_r, ring2_r,
    side_s, mate_s, fwd_s, back_s, relay_s, pair_s, ring1_s, direct_s, ring2_s, next_s, out_s, keep_s,
    tail_r, tail_s, tail_fwd_s, tail_keep_s, tail_mate_s,
):
    groups, blocks, rows, width = x_hbm.shape
    half = width // 2
    chips = n_tp // CORES
    stage = lax.axis_index("stage")
    rank = lax.axis_index("tp")
    chip, core = rank // CORES, lax.rem(rank, CORES)
    first = stage == 0
    final = stage == n_stage - 1
    gathers = jnp.where(first, groups - TAIL, groups)

    def at_chip(step):
        return lax.rem(chip + step, chips)

    right_c, left_c, opp_c = at_chip(1), at_chip(chips - 1), at_chip(2)
    mate = {"tp": chip * CORES + (1 - core)}
    right = {"tp": right_c * CORES + core}
    left = {"tp": left_c * CORES + core}
    ahead = {"stage": lax.rem(stage + 1, n_stage)}
    behind = {"stage": lax.rem(stage + n_stage - 1, n_stage)}
    block_r, block_l, block_o = right_c * CORES + core, left_c * CORES + core, opp_c * CORES + core
    cols = (pl.ds(0, half), pl.ds(half, half))

    def remote(src, dst, send, recv, device):
        return pltpu.make_async_remote_copy(
            src_ref=src, dst_ref=dst, send_sem=send, recv_sem=recv, device_id=device, device_id_type=MESH
        )

    def when_group(g):
        return pl.when((g >= 0) & (g < groups))

    def when_gathered(g):
        return pl.when((g >= 0) & (g < gathers))

    def is_tail(g):
        return final & (g >= groups - TAIL)

    def when_tail(g):
        return pl.when(final & (g >= groups - TAIL) & (g < groups))

    barrier = pltpu.get_barrier_semaphore()
    for peer in (mate, right, left, ahead, behind):
        pl.semaphore_signal(barrier, inc=1, device_id=peer, device_id_type=MESH)

    load_up = pltpu.make_async_copy(up_hbm.at[0], up, w_sem.at[0])
    load_down = pltpu.make_async_copy(down_hbm.at[0], down, w_sem.at[1])
    load_up.start()

    def load_x(g):
        return pltpu.make_async_copy(x_hbm.at[g], acts.at[groups + lax.rem(g, STAGING)], x_sem.at[lax.rem(g, STAGING)])

    @pl.when(first)
    def _():
        load_x(0).start()

    load_down.start()
    pl.semaphore_wait(barrier, 5)

    def in_slot(g):
        return jnp.where(first, groups + lax.rem(g, STAGING), g)

    def side_copy(g, way, h):
        ref = acts.at[g, rank, :, cols[h]]
        return remote(ref, ref, side_s.at[lax.rem(g, 4), way, h], side_r.at[lax.rem(g, 4), way, h], (right, left)[way])

    def fwd_copy(g, way):
        block = (block_l, block_r)[way]
        ref = acts.at[g, block, :, cols[way]]
        return remote(ref, ref, fwd_s.at[lax.rem(g, 4), way], opp_r.at[lax.rem(g, 4), way], (right, left)[way])

    def mate_copy(g, which):
        block = (rank, block_l, block_r, block_o)[which]
        return remote(acts.at[g, block], acts.at[g, block], mate_s.at[lax.rem(g, 4), which], mate_r.at[lax.rem(g, 4), which], mate)

    def back_copy(g, which):
        block = (block_l, block_r, block_o)[which]
        return remote(acts.at[g, block], y_hbm.at[g, block], back_s.at[lax.rem(g, 4), which], back_r.at[lax.rem(g, 4), which], behind)

    def next_copy(g):
        slot = lax.rem(g, 2)
        return remote(shard.at[slot], acts.at[g, rank], next_s.at[slot], own_r.at[lax.rem(g, 4)], ahead)

    def gather_own(g):
        @when_gathered(g)
        def _():
            next_copy(g).wait_recv()
            side_copy(g, 0, 0).start()
            side_copy(g, 1, 1).start()
            side_copy(g, 0, 1).start()
            side_copy(g, 1, 0).start()

            @pl.when(jnp.logical_not(first))
            def _():
                mate_copy(g, 0).start()

    def gather_sides(g):
        @when_gathered(g)
        def _():
            for way in range(2):
                side_copy(g, way, way).wait_recv()
                fwd_copy(g, way).start()

    def gather_rest(g):
        @when_gathered(g)
        def _():
            for way in range(2):
                side_copy(g, way, 1 - way).wait_recv()

            @pl.when(jnp.logical_not(first))
            def _():
                mate_copy(g, 1).start()
                mate_copy(g, 2).start()

            back_copy(g, 0).start()
            back_copy(g, 1).start()

    def gather_opposite(g):
        @when_gathered(g)
        def _():
            fwd_copy(g, 0).wait_recv()
            fwd_copy(g, 1).wait_recv()

            @pl.when(jnp.logical_not(first))
            def _():
                mate_copy(g, 3).start()

            back_copy(g, 2).start()

    def gather_mate(g):
        @pl.when((g >= 0) & (g < groups) & jnp.logical_not(first))
        def _():
            for which in range(4):
                mate_copy(g, which).wait_recv()

    def gather_sent(g):
        @when_gathered(g)
        def _():
            for way in range(2):
                side_copy(g, way, 0).wait_send()
                side_copy(g, way, 1).wait_send()
                fwd_copy(g, way).wait_send()
            for which in range(3):
                back_copy(g, which).wait_send()

            @pl.when(jnp.logical_not(first))
            def _():
                for which in range(4):
                    mate_copy(g, which).wait_send()

    def pair_copy(g, h):
        slot, to = lax.rem(g, 2), lax.rem(g, SLOTS)
        return remote(
            part.at[slot, 1 - core, :, :, cols[h]], pair.at[to, :, :, cols[h]], pair_s.at[slot, h], pair_r.at[to, h], mate
        )

    def ring1_copy(g, h):
        slot, to = lax.rem(g, 2), lax.rem(g, SLOTS)
        return remote(lead.at[slot, h, 0], ring1.at[to, h], ring1_s.at[slot, h], ring1_r.at[to, h], (right, left)[h])

    def direct_copy(g, h):
        slot, to = lax.rem(g, 2), lax.rem(g, SLOTS)
        return remote(lead.at[slot, h, 1], direct.at[to, h], direct_s.at[slot, h], direct_r.at[to, h], (left, right)[h])

    def ring2_copy(g, h):
        slot, to = lax.rem(g, 2), lax.rem(g, SLOTS)
        return remote(carry.at[slot, h], ring2.at[to, h], ring2_s.at[slot, h], ring2_r.at[to, h], (right, left)[h])

    def pair_sum(g, c, h):
        return part[lax.rem(g, 2), core, c, :, cols[h]].astype(F32) + pair[lax.rem(g, SLOTS), c, :, cols[h]].astype(F32)

    def reduce_pair(g, h):
        @when_group(g)
        def _():
            slot = lax.rem(g, 2)
            pair_copy(g, h).wait_recv()
            lead[slot, h, 0] = pair_sum(g, opp_c, h).astype(BF16)
            lead[slot, h, 1] = pair_sum(g, (left_c, right_c)[h], h).astype(BF16)
            ring1_copy(g, h).start()
            direct_copy(g, h).start()

    def reduce_ring(g, h):
        @when_group(g)
        def _():
            slot = lax.rem(g, 2)
            ring1_copy(g, h).wait_recv()
            total = pair_sum(g, (right_c, left_c)[h], h) + ring1[lax.rem(g, SLOTS), h].astype(F32)
            carry[slot, h] = total.astype(BF16)
            ring2_copy(g, h).start()

    def tail_side_copy(g, way):
        index = g - (groups - TAIL)
        return remote(
            shard.at[lax.rem(g, 2)], acts.at[g + TAIL, rank], tail_s.at[index, way], tail_r.at[index, way], (right, left)[way]
        )

    def tail_fwd_copy(g, way):
        index = g - (groups - TAIL)
        ref = acts.at[g + TAIL, (block_l, block_r)[way], :, cols[way]]
        return remote(ref, ref, tail_fwd_s.at[index, way], tail_r.at[index, 2 + way], (right, left)[way])

    def tail_keep_copy(g, which):
        index, block = g - (groups - TAIL), (block_l, block_r, block_o)[which]
        return pltpu.make_async_copy(acts.at[g + TAIL, block], y_hbm.at[g, block], tail_keep_s.at[index, which])

    def tail_mate_copy(g, which):
        index, block = g - (groups - TAIL), (block_l, block_r, block_o)[which]
        return remote(acts.at[g + TAIL, block], y_hbm.at[g, block], tail_mate_s.at[index, which], relay_r.at[lax.rem(g, 8), which], mate)

    def tail_own(g):
        @when_tail(g)
        def _():
            tail_side_copy(g, 0).start()
            tail_side_copy(g, 1).start()

    def tail_sides(g):
        @when_tail(g)
        def _():
            for way in range(2):
                tail_side_copy(g, way).wait_recv()
                tail_fwd_copy(g, way).start()
            for which in range(2):
                tail_mate_copy(g, which).start()
                tail_keep_copy(g, which).start()

    def tail_opposite(g):
        @when_tail(g)
        def _():
            for way in range(2):
                tail_fwd_copy(g, way).wait_recv()
            tail_mate_copy(g, 2).start()
            tail_keep_copy(g, 2).start()

    def tail_start(i):
        @pl.when(i == groups)
        def _():
            tail_own(i - 2)

    def tail_finish(i):
        @pl.when(i == groups)
        def _():
            tail_own(i - 1)
            for back in (2, 1):
                tail_sides(i - back)
            for back in (2, 1):
                tail_opposite(i - back)

    def tail_done(g):
        @when_tail(g)
        def _():
            for way in range(2):
                tail_fwd_copy(g, way).wait_send()
            for which in range(3):
                tail_mate_copy(g, which).wait_send()
                tail_keep_copy(g, which).wait()

    def keep_copy(g):
        slot = lax.rem(g, 2)
        return pltpu.make_async_copy(shard.at[slot], y_hbm.at[g, rank], keep_s.at[slot])

    def out_copy(g):
        slot = lax.rem(g, 2)
        return remote(shard.at[slot], y_hbm.at[g, rank], out_s.at[slot], out_r.at[lax.rem(g, 8)], mate)

    def reduce_last(g):
        @when_group(g)
        def _():
            slot = lax.rem(g, 2)
            for h in range(2):
                direct_copy(g, h).wait_recv()
                ring2_copy(g, h).wait_recv()
            src = in_slot(g)
            for h in range(2):
                total = pair_sum(g, chip, h) + ring2[lax.rem(g, SLOTS), h].astype(F32) + direct[lax.rem(g, SLOTS), h].astype(F32)
                shard[slot, :, cols[h]] = (acts[src, rank, :, cols[h]].astype(F32) + total).astype(BF16)
            @pl.when(jnp.logical_not(is_tail(g)))
            def _():
                next_copy(g).start()

            keep_copy(g).start()
            out_copy(g).start()

    def reduce_sent(g):
        @when_group(g)
        def _():
            for h in range(2):
                pair_copy(g, h).wait_send()
                ring1_copy(g, h).wait_send()
                direct_copy(g, h).wait_send()

    def shard_sent(g):
        @when_group(g)
        def _():
            for h in range(2):
                ring2_copy(g, h).wait_send()

            @pl.when(jnp.logical_not(is_tail(g)))
            def _():
                next_copy(g).wait_send()

            @pl.when(is_tail(g))
            def _():
                tail_side_copy(g, 0).wait_send()
                tail_side_copy(g, 1).wait_send()

            keep_copy(g).wait()
            out_copy(g).wait_send()

    def relay_copy(g, which):
        block = (block_l, block_r, block_o)[which]
        ref = y_hbm.at[g, block]
        return remote(ref, ref, relay_s.at[lax.rem(g, 4), which], relay_r.at[lax.rem(g, 8), which], mate)

    def relay(g):
        @pl.when((g >= 0) & (g < groups) & jnp.logical_not(is_tail(g)))
        def _():
            for which in range(3):
                back_copy(g, which).wait_recv()
                relay_copy(g, which).start()

    def relay_done(g):
        @when_group(g)
        def _():
            for which in range(3):
                relay_copy(g, which).wait_recv()

                @pl.when(jnp.logical_not(is_tail(g)))
                def _():
                    relay_copy(g, which).wait_send()

            out_copy(g).wait_recv()

    def layer_norm(g):
        src = in_slot(g)
        gain = gain_ref[...].astype(F32)
        per = LN_ROWS // rows
        for piece in range(blocks // per):
            y = acts[src, pl.ds(piece * per, per)].reshape(LN_ROWS, width).astype(F32)
            centered = y - jnp.mean(y, axis=-1, keepdims=True)
            variance = jnp.mean(centered * centered, axis=-1, keepdims=True)
            normed[pl.ds(piece * LN_ROWS, LN_ROWS), :] = (centered * lax.rsqrt(variance + EPS) * gain).astype(BF16)

    def matmul_up(piece):
        part_cols = pl.ds(piece * (hidden.shape[1] // UP_PIECES), hidden.shape[1] // UP_PIECES)
        total = jnp.dot(normed[...], up[:, part_cols], preferred_element_type=F32)
        hidden[:, part_cols] = jax.nn.gelu(total, approximate=True).astype(BF16)

    def matmul_down(g, h):
        slot = lax.rem(g, 2)
        total = jnp.dot(hidden[...], down[:, cols[h]], preferred_element_type=F32).astype(BF16)
        for block in range(blocks):
            part[slot, block % CORES, block // CORES, :, cols[h]] = total[block * rows:(block + 1) * rows]
        pair_copy(g, h).start()

    gather_lag = jnp.where(first, -LAG_FIRST, 2)

    def compute_norm(i):
        @when_group(i)
        def _():
            @pl.when(first)
            def _():
                load_x(i).wait()

                @pl.when(i + 1 < groups)
                def _():
                    load_x(i + 1).start()

            layer_norm(i)

    def compute_up(i, piece):
        @when_group(i)
        def _():
            @pl.when(i == 0)
            def _():
                if piece == 0:
                    load_up.wait()

            matmul_up(piece)

    def compute_down(i, h):
        @when_group(i)
        def _():
            @pl.when(i == 0)
            def _():
                if h == 0:
                    load_down.wait()

            matmul_down(i, h)

    def step(i):
        ag = i + gather_lag
        reduce_sent(i - 2)
        shard_sent(i - 3)
        gather_sent(ag - 4)
        relay(i - LAG_RELAY)
        relay_done(i - LAG_RELAY - 2)
        tail_done(i - 4)
        actions = {
            "mate": lambda: gather_mate(ag - 2),
            "norm": lambda: compute_norm(i),
            "up0": lambda: compute_up(i, 0),
            "down0": lambda: compute_down(i, 0),
            "down1": lambda: compute_down(i, 1),
            "pair0": lambda: reduce_pair(i, 0),
            "pair1": lambda: reduce_pair(i, 1),
            "ring0": lambda: reduce_ring(i - 1, 0),
            "ring1": lambda: (reduce_ring(i - 1, 1), tail_start(i)),
            "last": lambda: (reduce_last(i - 1), tail_finish(i)),
            "own": lambda: gather_own(ag - 1),
            "sides": lambda: gather_sides(ag - 1),
            "rest": lambda: gather_rest(ag - 1),
            "opp": lambda: gather_opposite(ag - 1),
        }
        for name in ORDER:
            actions[name]()

    @pl.loop(-2, groups + jnp.where(first, LAG_FIRST + 5 - TAIL, LAG_RELAY + 3))
    def _(i):
        step(i)


def keep_kernel(src, dst, held, in_sem, out_sem):
    groups = src.shape[0]
    reads = [pltpu.make_async_copy(src.at[g], held.at[g], in_sem.at[g]) for g in range(groups)]
    writes = [pltpu.make_async_copy(held.at[g], dst.at[g], out_sem.at[g]) for g in range(groups)]
    for copy in reads:
        copy.start()
    for g in range(groups):
        reads[g].wait()
        writes[g].start()
    for copy in writes:
        copy.wait()


def solution(mesh):
    n_stage = mesh.shape["stage"]
    n_tp = mesh.shape["tp"]

    def per_device(x_local, gain_local, up_local, down_local):
        micro, tokens, width = x_local.shape
        inner = up_local.shape[2]
        groups, size = micro // MERGE, MERGE * tokens
        rows = size // n_tp
        chips = n_tp // CORES
        half = width // 2
        x_blocks = x_local.reshape(groups, n_tp, rows, width)
        dma = pltpu.SemaphoreType.DMA
        out = pl.pallas_call(
            functools.partial(mlp_kernel, n_stage, n_tp),
            out_shape=jax.ShapeDtypeStruct(x_blocks.shape, BF16),
            in_specs=[
                pl.BlockSpec(memory_space=pl.ANY),
                pl.BlockSpec(memory_space=pltpu.VMEM),
                pl.BlockSpec(memory_space=pl.ANY),
                pl.BlockSpec(memory_space=pl.ANY),
            ],
            out_specs=pl.BlockSpec(memory_space=pl.ANY),
            scratch_shapes=[
                pltpu.VMEM((width, inner), BF16),
                pltpu.VMEM((inner, width), BF16),
                pltpu.VMEM((groups + STAGING, n_tp, rows, width), BF16),
                pltpu.VMEM((size, width), BF16),
                pltpu.VMEM((size, inner), BF16),
                pltpu.VMEM((2, CORES, chips, rows, width), BF16),
                pltpu.VMEM((SLOTS, chips, rows, width), BF16),
                pltpu.VMEM((2, 2, 2, rows, half), BF16),
                pltpu.VMEM((SLOTS, 2, rows, half), BF16),
                pltpu.VMEM((SLOTS, 2, rows, half), BF16),
                pltpu.VMEM((SLOTS, 2, rows, half), BF16),
                pltpu.VMEM((2, 2, rows, half), BF16),
                pltpu.VMEM((2, rows, width), BF16),
                dma((2,)), dma((STAGING,)),
                dma((4,)), dma((4, 2, 2)), dma((4, 2)), dma((4, 4)),
                dma((4, 3)), dma((8, 3)), dma((8,)),
                dma((SLOTS, 2)), dma((SLOTS, 2)), dma((SLOTS, 2)), dma((SLOTS, 2)),
                dma((4, 2, 2)), dma((4, 4)), dma((4, 2)), dma((4, 3)), dma((4, 3)),
                dma((2, 2)), dma((2, 2)), dma((2, 2)), dma((2, 2)), dma((2,)), dma((2,)), dma((2,)),
                dma((TAIL, 4)), dma((TAIL, 2)), dma((TAIL, 2)), dma((TAIL, 3)), dma((TAIL, 3)),
            ],
            compiler_params=pltpu.CompilerParams(
                collective_id=0, has_side_effects=True, vmem_limit_bytes=66_000_000
            ),
            name="mlp_pipeline",
        )(x_blocks, gain_local, up_local, down_local)
        kept = pl.pallas_call(
            keep_kernel,
            out_shape=jax.ShapeDtypeStruct(x_blocks.shape, BF16),
            in_specs=[pl.BlockSpec(memory_space=pl.ANY)],
            out_specs=pl.BlockSpec(memory_space=pl.ANY),
            scratch_shapes=[pltpu.VMEM(x_blocks.shape, BF16), dma((groups,)), dma((groups,))],
            compiler_params=pltpu.CompilerParams(vmem_limit_bytes=40_000_000),
            name="keep_result",
        )(out)
        return kept.reshape(1, micro, tokens, width)

    return jax.shard_map(per_device, mesh=mesh, in_specs=(P("data"), P("stage"), P("stage", None, "tp"), P("stage", "tp", None)), out_specs=P("stage", "data"), check_vma=False)
```
